32 devices in a mesh: rows: 8 (over z, x), tp: 2 (over core), job: 2 (over y).
Axes of the slice: x: 2, y: 2, z: 4, core: 2. Of those that a mesh axis runs over, the one named last changes fastest.
Arguments:
- train_query: bfloat16 [4096, 2048], P(('job', 'rows'), 'tp'), parts along dimension 0, may hold values from -0.125 to 0.125
- low_query: bfloat16 [4096, 16], P(('job', 'rows')), parts along dimension 0, may hold values from -0.125 to 0.125
- high_query: bfloat16 [32, 2048], P('job', 'tp'), parts along dimension 0, may hold values from -1.5 to 1.5
- train_key: bfloat16 [4096, 512], P(('job', 'rows'), 'tp'), parts along dimension 0, may hold values from -0.125 to 0.125
- low_key: bfloat16 [4096, 16], P(('job', 'rows')), parts along dimension 0, may hold values from -0.125 to 0.125
- high_key: bfloat16 [32, 512], P('job', 'tp'), parts along dimension 0, may hold values from -1.5 to 1.5
- train_value: bfloat16 [4096, 512], P(('job', 'rows'), 'tp'), parts along dimension 0, may hold values from -0.125 to 0.125
- low_value: bfloat16 [4096, 16], P(('job', 'rows')), parts along dimension 0, may hold values from -0.125 to 0.125
- high_value: bfloat16 [32, 512], P('job', 'tp'), parts along dimension 0, may hold values from -1.5 to 1.5
- norm_train: float32 [4096], P(('job', 'rows', 'tp')), parts along dimension 0, may hold values from 0.25 to 1.75
- norm_step: float32 [4096], P(('job', 'rows', 'tp')), parts along dimension 0, may hold values from -0.3 to 0.3
Outputs:
- serve_query: bfloat16 [4096, 2048], P(('job', 'tp')), parts along dimension 0
- serve_key: bfloat16 [1024, 2048], P(('job', 'tp')), parts along dimension 0
- serve_value: bfloat16 [1024, 2048], P(('job', 'tp')), parts along dimension 0
- serve_norm: bfloat16 [4096], P('job'), parts along dimension 0
The draws below stay inside these ranges and needn't reach their ends.
There are 2 independent parts, one for each index of `job`. The reference program is written for one: setup_inputs(seed, part) draws one part's arguments, and reference() takes and returns one part's arrays. A program takes and returns all parts, laid end to end along the dimension named above; each array names one. Nothing has to cross between parts.
All inputs are finite; a program needn't handle non-finite values.
Results may differ from the reference program's by a relative error of at most 0.001.
Values may be sent and summed in bfloat16 or wider, within the bound.
A program may use at most 64 MiB of HBM per device.

```python
import jax
import jax.numpy as jnp

D_MODEL = 2048
Q_DIM = 2048
KV_DIM = 512
RANK = 16


def level_of(stream_key, extent, pieces, low, top_value):
    gain = 1.0
    for dim, blocks in pieces:
        heights = jax.random.uniform(jax.random.fold_in(jax.random.fold_in(stream_key, 6), dim), (blocks,), jnp.float32, low / len(pieces), top_value / len(pieces))
        gain = gain * jnp.repeat(jnp.exp(heights), extent[dim] // blocks).reshape((-1,) + (1,) * (len(extent) - 1 - dim))
    return gain


def centred(own_key, shape, spread, reach, cuts=(), kind=jnp.bfloat16):
    entries = spread * jax.random.normal(own_key, shape, jnp.float32)
    if cuts:
        entries = entries * level_of(own_key, shape, cuts, -0.22, 0.18)
    return jnp.clip(entries, -reach, reach).astype(kind)


def setup_inputs(seed: int = 0, part: int = 0) -> dict:
    key_of = jax.random.split(jax.random.key(seed), 12)
    own_keys = jax.random.split(jax.random.fold_in(key_of[11], part), 12)
    return {
        "train_query": centred(own_keys[0], (D_MODEL, Q_DIM), D_MODEL ** -0.5, 0.125, ((0, 8), (1, 2))),
        "low_query": centred(own_keys[1], (D_MODEL, RANK), D_MODEL ** -0.5, 0.125, ((0, 8),)),
        "high_query": centred(own_keys[2], (RANK, Q_DIM), RANK ** -0.5, 1.5, ((1, 2),)),
        "train_key": centred(own_keys[3], (D_MODEL, KV_DIM), D_MODEL ** -0.5, 0.125, ((0, 8), (1, 2))),
        "low_key": centred(own_keys[4], (D_MODEL, RANK), D_MODEL ** -0.5, 0.125, ((0, 8),)),
        "high_key": centred(own_keys[5], (RANK, KV_DIM), RANK ** -0.5, 1.5, ((1, 2),)),
        "train_value": centred(own_keys[6], (D_MODEL, KV_DIM), D_MODEL ** -0.5, 0.125, ((0, 8), (1, 2))),
        "low_value": centred(own_keys[7], (D_MODEL, RANK), D_MODEL ** -0.5, 0.125, ((0, 8),)),
        "high_value": centred(own_keys[8], (RANK, KV_DIM), RANK ** -0.5, 1.5, ((1, 2),)),
        "norm_train": jnp.clip(1.0 + 0.15 * jax.random.normal(own_keys[9], (D_MODEL,), jnp.float32), 0.25, 1.75),
        "norm_step": jnp.clip(jax.random.uniform(own_keys[10], (D_MODEL,), jnp.float32, -0.3, 0.3) * level_of(own_keys[10], (D_MODEL,), ((0, 16),), -0.4, 0.0), -0.3, 0.3),
    }


mix_rate = 0.5


def reference(train_query, low_query, high_query, train_key, low_key, high_key, train_value, low_value, high_value, norm_train, norm_step):
    fresh_query = train_query.astype(jnp.float32) + mix_rate * jnp.dot(low_query, high_query, preferred_element_type=jnp.float32)
    fresh_key = train_key.astype(jnp.float32) + mix_rate * jnp.dot(low_key, high_key, preferred_element_type=jnp.float32)
    fresh_value = train_value.astype(jnp.float32) + mix_rate * jnp.dot(low_value, high_value, preferred_element_type=jnp.float32)
    serve_query = fresh_query.T.astype(jnp.bfloat16)
    serve_key = fresh_key.T.astype(jnp.bfloat16)
    serve_value = fresh_value.T.astype(jnp.bfloat16)
    serve_norm = (norm_train + norm_step).astype(jnp.bfloat16)
    return serve_query, serve_key, serve_value, serve_norm
```

```python
import functools

import jax
import jax.numpy as jnp
from jax import lax
from jax.experimental import pallas as pl
from jax.experimental.pallas import tpu as pltpu
from jax.sharding import PartitionSpec as P

mix_rate = 0.5
CHUNK_ROWS = 128
MESH = pl.DeviceIdType.MESH


def kernel(
    size,
    tp_size,
    *refs,
):
    given, refs = refs[:11], refs[11:]
    serve_query, serve_key, serve_value, serve_norm = refs[:4]
    held, refs = refs[4:15], refs[15:]
    run_kernel(size, tp_size, given, held, serve_query, serve_key, serve_value, serve_norm, *refs)


def run_kernel(
    size,
    tp_size,
    given,
    held,
    serve_query,
    serve_key,
    serve_value,
    serve_norm,
    gains,
    load_sem,
    send_sem,
    recv_sem,
    gain_send,
    gain_recv,
):
    loads = [
        pltpu.make_async_copy(g, h, load_sem.at[n]) for n, (g, h) in enumerate(zip(given, held))
    ]
    for load in loads:
        load.start()
    (
        train_query,
        low_query,
        high_query,
        train_key,
        low_key,
        high_key,
        train_value,
        low_value,
        high_value,
        norm_train,
        norm_step,
    ) = held
    depth = size // 2
    me = lax.axis_index("rows")
    core = lax.axis_index("tp")
    z, x = me // 2, lax.rem(me, 2)
    other = 1 - x
    width = train_query.shape[0]
    up, down, side = me + 2, me - 2, 2 * z + other
    targets = (up, down, side)
    has_up, has_down = z < depth - 1, z > 0
    UP, DOWN, SIDE = 0, 1, 2

    seats = size * tp_size
    seat = me * tp_size + core

    def peer(k):
        p = lax.rem(seat + k, seats)
        return {"rows": p // tp_size, "tp": lax.rem(p, tp_size)}

    barrier = pltpu.get_barrier_semaphore()
    for k in range(1, seats):
        pl.semaphore_signal(barrier, inc=1, device_id=peer(k), device_id_type=MESH)

    chunks = []
    for train, low, high, serve in (
        (train_query, low_query, high_query, serve_query),
        (train_key, low_key, high_key, serve_key),
        (train_value, low_value, high_value, serve_value),
    ):
        for start in range(0, serve.shape[0], CHUNK_ROWS):
            chunks.append((train, low, high, serve, start))
    count = len(chunks)

    def piece(item, c):
        serve, start = chunks[c][3], chunks[c][4]
        return serve.at[
            pl.ds(start, CHUNK_ROWS), pl.ds(pl.multiple_of(item * width, 128), width)
        ]

    def copy(item, c, way):
        ref = piece(item, c)
        return pltpu.make_async_remote_copy(
            src_ref=ref,
            dst_ref=ref,
            send_sem=send_sem.at[way, item, c],
            recv_sem=recv_sem.at[item, c],
            device_id={"rows": targets[way]},
            device_id_type=MESH,
        )

    def arrive(item, c):
        copy(item, c, SIDE).wait_recv()

    def crossing(c):
        return c % 2 == 1

    def merge(c):
        train, low, high, serve, start = chunks[c]
        rows = pl.ds(start, CHUNK_ROWS)
        update = lax.dot_general(
            high[:, rows], low[...], (((0,), (0,)), ((), ())), preferred_element_type=jnp.float32
        )
        fresh = train[:, rows].T.astype(jnp.float32) + mix_rate * update
        serve[rows, pl.ds(pl.multiple_of(me * width, 128), width)] = fresh.astype(jnp.bfloat16)

    def send_own(c):
        @pl.when(has_down)
        def _():
            copy(me, c, DOWN).start()

        @pl.when(has_up)
        def _():
            copy(me, c, UP).start()

        copy(me, c, SIDE).start()

    def gain_copy(k):
        return pltpu.make_async_remote_copy(
            src_ref=gains.at[seat],
            dst_ref=gains.at[seat],
            send_sem=gain_send.at[k],
            recv_sem=gain_recv.at[k],
            device_id=peer(k),
            device_id_type=MESH,
        )

    for load in loads:
        load.wait()
    gains[pl.ds(seat, 1)] = (norm_train[...] + norm_step[...])[None]
    merge(0)
    merge(1)
    pl.semaphore_wait(barrier, seats - 1)
    for c in range(2, count + 2):
        send_own(c - 2)
        if c < count:
            merge(c)
    for k in range(1, seats):
        gain_copy(k).start()

    def pass_on(step, c):
        below, above = me - 2 * step, me + 2 * step

        @pl.when(z >= step)
        def _():
            arrive(below, c)

            @pl.when(has_up)
            def _():
                copy(below, c, UP).start()

            if not (step == 1 and crossing(c)):
                copy(below, c, SIDE).start()

        @pl.when(z + step < depth)
        def _():
            arrive(above, c)

            @pl.when(has_down)
            def _():
                copy(above, c, DOWN).start()

            if not (step == 1 and crossing(c)):
                copy(above, c, SIDE).start()

    def cross(c):
        arrive(side, c)

        @pl.when(has_down)
        def _():
            copy(side, c, DOWN).start()

        @pl.when(has_up)
        def _():
            copy(side, c, UP).start()

    for step in range(1, depth):
        for c in range(count):
            pass_on(step, c)
        if step == max(1, depth - 2):
            for c in range(count):
                if crossing(c):
                    cross(c)

    for c in range(count):
        if not crossing(c):
            arrive(side, c)
    for step in range(1, depth):
        for c in range(count):
            @pl.when(z >= step)
            def _():
                arrive(side - 2 * step, c)

            @pl.when(z + step < depth)
            def _():
                arrive(side + 2 * step, c)

    for k in range(1, seats):
        gain_copy(k).wait_recv()
    serve_norm[...] = gains[...].reshape(serve_norm.shape).astype(jnp.bfloat16)

    for k in range(1, seats):
        gain_copy(k).wait_send()
    for c in range(count):
        copy(me, c, SIDE).wait_send()

        @pl.when(has_down)
        def _():
            copy(me, c, DOWN).wait_send()
            if crossing(c):
                copy(side, c, DOWN).wait_send()

        @pl.when(has_up)
        def _():
            copy(me, c, UP).wait_send()
            if crossing(c):
                copy(side, c, UP).wait_send()

        for step in range(1, depth):
            below, above = me - 2 * step, me + 2 * step

            @pl.when(z >= step)
            def _():
                @pl.when(has_up)
                def _():
                    copy(below, c, UP).wait_send()

                if not (step == 1 and crossing(c)):
                    copy(below, c, SIDE).wait_send()

            @pl.when(z + step < depth)
            def _():
                @pl.when(has_down)
                def _():
                    copy(above, c, DOWN).wait_send()

                if not (step == 1 and crossing(c)):
                    copy(above, c, SIDE).wait_send()


def fused(size, tp_size, *args):
    train_query, train_key, train_value, norm_train = args[0], args[3], args[6], args[9]
    seats, norm_length = size * tp_size, norm_train.shape[0]
    args = [a.T if n in (1, 4, 7) else a for n, a in enumerate(args)]
    args = [a.reshape(1, -1) if a.ndim == 1 else a for a in args]
    full = train_query.shape[0] * size
    outs = [
        pltpu.VMEM((t.shape[1], full), jnp.bfloat16)
        for t in (train_query, train_key, train_value)
    ]
    outs.append(pltpu.VMEM((seats, norm_length), jnp.bfloat16))
    count = sum(t.shape[1] for t in (train_query, train_key, train_value)) // CHUNK_ROWS
    vmem = pl.BlockSpec(memory_space=pltpu.VMEM)
    query, key, value, norm = pl.pallas_call(
        functools.partial(kernel, size, tp_size),
        out_shape=outs,
        in_specs=[pl.BlockSpec(memory_space=pltpu.HBM)] * 11,
        out_specs=[vmem] * 4,
        scratch_shapes=[pltpu.VMEM(a.shape, a.dtype) for a in args]
        + [
            pltpu.VMEM((seats, 1, norm_length), jnp.float32),
            pltpu.SemaphoreType.DMA((11,)),
            pltpu.SemaphoreType.DMA((3, size, count)),
            pltpu.SemaphoreType.DMA((size, count)),
            pltpu.SemaphoreType.DMA((seats,)),
            pltpu.SemaphoreType.DMA((seats,)),
        ],
        compiler_params=pltpu.CompilerParams(
            collective_id=0, has_side_effects=True, vmem_limit_bytes=16 * 2**20
        ),
    )(*args)
    query, key, value, norm = store_out(query, key, value, norm)
    return query, key, value, norm.reshape(-1)


def store_kernel(*refs):
    ins, outs, sems = refs[:4], refs[4:8], refs[8]
    copies = [pltpu.make_async_copy(i, o, sems.at[n]) for n, (i, o) in enumerate(zip(ins, outs))]
    for c in copies:
        c.start()
    for c in copies:
        c.wait()


def store_out(*arrays):
    return pl.pallas_call(
        store_kernel,
        out_shape=[jax.ShapeDtypeStruct(a.shape, a.dtype) for a in arrays],
        in_specs=[pl.BlockSpec(memory_space=pltpu.VMEM)] * 4,
        out_specs=[pl.BlockSpec(memory_space=pltpu.HBM)] * 4,
        scratch_shapes=[pltpu.SemaphoreType.DMA((4,))],
        compiler_params=pltpu.CompilerParams(vmem_limit_bytes=16 * 2**20),
    )(*arrays)


def plain(
    train_query,
    low_query,
    high_query,
    train_key,
    low_key,
    high_key,
    train_value,
    low_value,
    high_value,
    norm_train,
    norm_step,
):
    def merged(train, low, high):
        update = jnp.dot(low, high, preferred_element_type=jnp.float32)
        fresh = train.astype(jnp.float32) + mix_rate * update
        return lax.all_gather(fresh.astype(jnp.bfloat16), "rows", axis=0, tiled=True).T

    serve_norm = lax.all_gather(
        (norm_train + norm_step).astype(jnp.bfloat16), ("rows", "tp"), axis=0, tiled=True
    )
    return (
        merged(train_query, low_query, high_query),
        merged(train_key, low_key, high_key),
        merged(train_value, low_value, high_value),
        serve_norm,
    )


def solution(mesh):
    size, tp_size = mesh.shape["rows"], mesh.shape["tp"]

    def local(*args):
        trains = (args[0], args[3], args[6])
        fits = (
            size % 2 == 0
            and size >= 4
            and all(t.shape[0] % 128 == 0 and t.shape[1] % CHUNK_ROWS == 0 for t in trains)
            and args[9].shape[0] % 128 == 0
        )
        return fused(size, tp_size, *args) if fits else plain(*args)

    in_specs = (
        P(("job", "rows"), "tp"),
        P(("job", "rows"), None),
        P("job", "tp"),
        P(("job", "rows"), "tp"),
        P(("job", "rows"), None),
        P("job", "tp"),
        P(("job", "rows"), "tp"),
        P(("job", "rows"), None),
        P("job", "tp"),
        P(("job", "rows", "tp")),
        P(("job", "rows", "tp")),
    )
    out_specs = (P(("job", "tp"), None), P(("job", "tp"), None), P(("job", "tp"), None), P("job"))
    return jax.shard_map(local, mesh=mesh, in_specs=in_specs, out_specs=out_specs, check_vma=False)
```

```python
import functools

import jax
import jax.numpy as jnp
from jax import lax
from jax.experimental import pallas as pl
from jax.experimental.pallas import tpu as pltpu
from jax.sharding import PartitionSpec as P

mix_rate = 0.5
CHUNK_ROWS = 256
VMEM_BYTES = 67043328
MESH = pl.DeviceIdType.MESH


def kernel(
    size,
    tp_size,
    *refs,
):
    given, refs = refs[:11], refs[11:]
    serve_query, serve_key, serve_value, serve_norm = refs[:4]
    held, refs = refs[4:15], refs[15:]
    run_kernel(size, tp_size, given, held, serve_query, serve_key, serve_value, serve_norm, *refs)


def run_kernel(
    size,
    tp_size,
    given,
    held,
    serve_query,
    serve_key,
    serve_value,
    serve_norm,
    gains,
    load_sem,
    send_sem,
    recv_sem,
    gain_send,
    gain_recv,
):
    loads = [
        pltpu.make_async_copy(g, h, load_sem.at[n]) for n, (g, h) in enumerate(zip(given, held))
    ]
    for load in loads:
        load.start()
    (
        train_query,
        low_query,
        high_query,
        train_key,
        low_key,
        high_key,
        train_value,
        low_value,
        high_value,
        norm_train,
        norm_step,
    ) = held
    depth = size // 2
    me = lax.axis_index("rows")
    core = lax.axis_index("tp")
    z, x = me // 2, lax.rem(me, 2)
    other = 1 - x
    width = train_query.shape[0]
    up, down, side = me + 2, me - 2, 2 * z + other
    targets = (up, down, side)
    has_up, has_down = z < depth - 1, z > 0
    UP, DOWN, SIDE = 0, 1, 2

    seats = size * tp_size
    seat = me * tp_size + core

    def peer(k):
        p = lax.rem(seat + k, seats)
        return {"rows": p // tp_size, "tp": lax.rem(p, tp_size)}

    barrier = pltpu.get_barrier_semaphore()
    for k in range(1, seats):
        pl.semaphore_signal(barrier, inc=1, device_id=peer(k), device_id_type=MESH)

    chunks = []
    for train, low, high, serve in (
        (train_query, low_query, high_query, serve_query),
        (train_key, low_key, high_key, serve_key),
        (train_value, low_value, high_value, serve_value),
    ):
        for start in range(0, serve.shape[0], CHUNK_ROWS):
            chunks.append((train, low, high, serve, start))
    count = len(chunks)

    def piece(item, c):
        serve, start = chunks[c][3], chunks[c][4]
        return serve.at[
            pl.ds(start, CHUNK_ROWS), pl.ds(pl.multiple_of(item * width, 128), width)
        ]

    def copy(item, c, way):
        ref = piece(item, c)
        return pltpu.make_async_remote_copy(
            src_ref=ref,
            dst_ref=ref,
            send_sem=send_sem.at[way, item, c],
            recv_sem=recv_sem.at[item, c],
            device_id={"rows": targets[way]},
            device_id_type=MESH,
        )

    def arrive(item, c):
        copy(item, c, SIDE).wait_recv()

    def crossing(c):
        return c % 2 == 1

    def merge(c):
        train, low, high, serve, start = chunks[c]
        rows = pl.ds(start, CHUNK_ROWS)
        update = lax.dot_general(
            high[:, rows], low[...], (((0,), (0,)), ((), ())), preferred_element_type=jnp.float32
        )
        fresh = train[:, rows].T.astype(jnp.float32) + mix_rate * update
        serve[rows, pl.ds(pl.multiple_of(me * width, 128), width)] = fresh.astype(jnp.bfloat16)

    def send_own(c):
        @pl.when(has_down)
        def _():
            copy(me, c, DOWN).start()

        @pl.when(has_up)
        def _():
            copy(me, c, UP).start()

        copy(me, c, SIDE).start()

    def gain_copy(k):
        return pltpu.make_async_remote_copy(
            src_ref=gains.at[seat],
            dst_ref=gains.at[seat],
            send_sem=gain_send.at[k],
            recv_sem=gain_recv.at[k],
            device_id=peer(k),
            device_id_type=MESH,
        )

    for load in loads:
        load.wait()
    gains[pl.ds(seat, 1)] = (norm_train[...] + norm_step[...])[None]
    merge(0)
    merge(1)
    pl.semaphore_wait(barrier, seats - 1)
    for c in range(2, count + 2):
        send_own(c - 2)
        if c < count:
            merge(c)
    for k in range(1, seats):
        gain_copy(k).start()

    def pass_on(step, c):
        below, above = me - 2 * step, me + 2 * step

        @pl.when(z >= step)
        def _():
            arrive(below, c)

            @pl.when(has_up)
            def _():
                copy(below, c, UP).start()

            if not (step == 1 and crossing(c)):
                copy(below, c, SIDE).start()

        @pl.when(z + step < depth)
        def _():
            arrive(above, c)

            @pl.when(has_down)
            def _():
                copy(above, c, DOWN).start()

            if not (step == 1 and crossing(c)):
                copy(above, c, SIDE).start()

    def cross(c):
        arrive(side, c)

        @pl.when(has_down)
        def _():
            copy(side, c, DOWN).start()

        @pl.when(has_up)
        def _():
            copy(side, c, UP).start()

    for step in range(1, depth):
        for c in range(count):
            pass_on(step, c)
        if step == max(1, depth - 2):
            for c in range(count):
                if crossing(c):
                    cross(c)

    for c in range(count):
        if not crossing(c):
            arrive(side, c)
    for step in range(1, depth):
        for c in range(count):
            @pl.when(z >= step)
            def _():
                arrive(side - 2 * step, c)

            @pl.when(z + step < depth)
            def _():
                arrive(side + 2 * step, c)

    for k in range(1, seats):
        gain_copy(k).wait_recv()
    serve_norm[...] = gains[...].reshape(serve_norm.shape).astype(jnp.bfloat16)

    for k in range(1, seats):
        gain_copy(k).wait_send()
    for c in range(count):
        copy(me, c, SIDE).wait_send()

        @pl.when(has_down)
        def _():
            copy(me, c, DOWN).wait_send()
            if crossing(c):
                copy(side, c, DOWN).wait_send()

        @pl.when(has_up)
        def _():
            copy(me, c, UP).wait_send()
            if crossing(c):
                copy(side, c, UP).wait_send()

        for step in range(1, depth):
            below, above = me - 2 * step, me + 2 * step

            @pl.when(z >= step)
            def _():
                @pl.when(has_up)
                def _():
                    copy(below, c, UP).wait_send()

                if not (step == 1 and crossing(c)):
                    copy(below, c, SIDE).wait_send()

            @pl.when(z + step < depth)
            def _():
                @pl.when(has_down)
                def _():
                    copy(above, c, DOWN).wait_send()

                if not (step == 1 and crossing(c)):
                    copy(above, c, SIDE).wait_send()


def fused(size, tp_size, *args):
    train_query, train_key, train_value, norm_train = args[0], args[3], args[6], args[9]
    seats, norm_length = size * tp_size, norm_train.shape[0]
    args = [a.T if n in (1, 4, 7) else a for n, a in enumerate(args)]
    args = [a.reshape(1, -1) if a.ndim == 1 else a for a in args]
    full = train_query.shape[0] * size
    outs = [
        pltpu.VMEM((t.shape[1], full), jnp.bfloat16)
        for t in (train_query, train_key, train_value)
    ]
    outs.append(pltpu.VMEM((seats, norm_length), jnp.bfloat16))
    count = sum(t.shape[1] for t in (train_query, train_key, train_value)) // CHUNK_ROWS
    grant = VMEM_BYTES - 2 * (sum(t.shape[1] for t in (train_query, train_key, train_value)) * full)
    grant -= 2 * seats * norm_length
    vmem = pl.BlockSpec(memory_space=pltpu.VMEM)
    query, key, value, norm = pl.pallas_call(
        functools.partial(kernel, size, tp_size),
        out_shape=outs,
        in_specs=[pl.BlockSpec(memory_space=pltpu.HBM)] * 11,
        out_specs=[vmem] * 4,
        scratch_shapes=[pltpu.VMEM(a.shape, a.dtype) for a in args]
        + [
            pltpu.VMEM((seats, 1, norm_length), jnp.float32),
            pltpu.SemaphoreType.DMA((11,)),
            pltpu.SemaphoreType.DMA((3, size, count)),
            pltpu.SemaphoreType.DMA((size, count)),
            pltpu.SemaphoreType.DMA((seats,)),
            pltpu.SemaphoreType.DMA((seats,)),
        ],
        compiler_params=pltpu.CompilerParams(
            collective_id=0, has_side_effects=True, vmem_limit_bytes=grant
        ),
    )(*args)
    query, key, value, norm = store_out(query, key, value, norm)
    return query, key, value, norm.reshape(-1)


def store_kernel(*refs):
    ins, outs, sems = refs[:4], refs[4:8], refs[8]
    copies = [pltpu.make_async_copy(i, o, sems.at[n]) for n, (i, o) in enumerate(zip(ins, outs))]
    for c in copies:
        c.start()
    for c in copies:
        c.wait()


def store_out(*arrays):
    return pl.pallas_call(
        store_kernel,
        out_shape=[jax.ShapeDtypeStruct(a.shape, a.dtype) for a in arrays],
        in_specs=[pl.BlockSpec(memory_space=pltpu.VMEM)] * 4,
        out_specs=[pl.BlockSpec(memory_space=pltpu.HBM)] * 4,
        scratch_shapes=[pltpu.SemaphoreType.DMA((4,))],
        compiler_params=pltpu.CompilerParams(vmem_limit_bytes=16 * 2**20),
    )(*arrays)


def plain(
    train_query,
    low_query,
    high_query,
    train_key,
    low_key,
    high_key,
    train_value,
    low_value,
    high_value,
    norm_train,
    norm_step,
):
    def merged(train, low, high):
        update = jnp.dot(low, high, preferred_element_type=jnp.float32)
        fresh = train.astype(jnp.float32) + mix_rate * update
        return lax.all_gather(fresh.astype(jnp.bfloat16), "rows", axis=0, tiled=True).T

    serve_norm = lax.all_gather(
        (norm_train + norm_step).astype(jnp.bfloat16), ("rows", "tp"), axis=0, tiled=True
    )
    return (
        merged(train_query, low_query, high_query),
        merged(train_key, low_key, high_key),
        merged(train_value, low_value, high_value),
        serve_norm,
    )


def solution(mesh):
    size, tp_size = mesh.shape["rows"], mesh.shape["tp"]

    def local(*args):
        trains = (args[0], args[3], args[6])
        fits = (
            size % 2 == 0
            and size >= 4
            and all(t.shape[0] % 128 == 0 and t.shape[1] % CHUNK_ROWS == 0 for t in trains)
            and args[9].shape[0] % 128 == 0
        )
        return fused(size, tp_size, *args) if fits else plain(*args)

    in_specs = (
        P(("job", "rows"), "tp"),
        P(("job", "rows"), None),
        P("job", "tp"),
        P(("job", "rows"), "tp"),
        P(("job", "rows"), None),
        P("job", "tp"),
        P(("job", "rows"), "tp"),
        P(("job", "rows"), None),
        P("job", "tp"),
        P(("job", "rows", "tp")),
        P(("job", "rows", "tp")),
    )
    out_specs = (P(("job", "tp"), None), P(("job", "tp"), None), P(("job", "tp"), None), P("job"))
    return jax.shard_map(local, mesh=mesh, in_specs=in_specs, out_specs=out_specs, check_vma=False)
```

```python
import functools

import jax
import jax.numpy as jnp
from jax import lax
from jax.experimental import pallas as pl
from jax.experimental.pallas import tpu as pltpu
from jax.sharding import PartitionSpec as P

mix_rate = 0.5
CHUNK_ROWS = 256
FIRST_ROWS = 256
VMEM_BYTES = 67043328
MESH = pl.DeviceIdType.MESH


def cuts(length, first):
    sizes = []
    while first and length > FIRST_ROWS and length % (2 * FIRST_ROWS) == 0:
        sizes.insert(0, min(length // 2, CHUNK_ROWS))
        length -= sizes[0]
    while length:
        sizes.insert(0, min(length, FIRST_ROWS if first else CHUNK_ROWS))
        length -= sizes[0]
    start, found = 0, []
    for rows in sizes:
        found.append((start, rows))
        start += rows
    return found


def kernel(
    size,
    tp_size,
    *refs,
):
    given, refs = refs[:11], refs[11:]
    serve_query, serve_key, serve_value, serve_norm = refs[:4]
    held, refs = refs[4:15], refs[15:]
    run_kernel(size, tp_size, given, held, serve_query, serve_key, serve_value, serve_norm, *refs)


def run_kernel(
    size,
    tp_size,
    given,
    held,
    serve_query,
    serve_key,
    serve_value,
    serve_norm,
    gains,
    load_sem,
    send_sem,
    recv_sem,
    gain_send,
    gain_recv,
):
    loads = [
        pltpu.make_async_copy(g, h, load_sem.at[n]) for n, (g, h) in enumerate(zip(given, held))
    ]
    (
        train_query,
        low_query,
        high_query,
        train_key,
        low_key,
        high_key,
        train_value,
        low_value,
        high_value,
        norm_train,
        norm_step,
    ) = held
    depth = size // 2
    me = lax.axis_index("rows")
    core = lax.axis_index("tp")
    z, x = me // 2, lax.rem(me, 2)
    other = 1 - x
    width = train_query.shape[0]
    up, down, side = me + 2, me - 2, 2 * z + other
    targets = (up, down, side)
    has_up, has_down = z < depth - 1, z > 0
    UP, DOWN, SIDE = 0, 1, 2

    def partner(k):
        return {"tp": lax.rem(core + k, tp_size)}

    barrier = pltpu.get_barrier_semaphore()

    def greet(device):
        pl.semaphore_signal(barrier, inc=1, device_id=device, device_id_type=MESH)

    @pl.when(has_up)
    def _():
        greet({"rows": up})

    @pl.when(has_down)
    def _():
        greet({"rows": down})

    greet({"rows": side})
    for k in range(1, tp_size):
        greet(partner(k))
    for load in loads:
        load.start()

    chunks = []
    for train, low, high, serve in (
        (train_query, low_query, high_query, serve_query),
        (train_key, low_key, high_key, serve_key),
        (train_value, low_value, high_value, serve_value),
    ):
        for start, rows in cuts(serve.shape[0], not chunks):
            chunks.append((train, low, high, serve, start, rows))
    count = len(chunks)
    queries = sum(c[3] is serve_query for c in chunks)
    twice, left = set(), sum(c[5] for c in chunks) // 2
    for c in sorted(range(count), key=lambda c: -chunks[c][5]):
        if chunks[c][5] <= left:
            twice.add(c)
            left -= chunks[c][5]

    def piece(item, c):
        if c == count:
            return gains.at[item]
        serve, start, rows = chunks[c][3:]
        return serve.at[pl.ds(start, rows), pl.ds(pl.multiple_of(item * width, 128), width)]

    def copy(item, c, way):
        ref = piece(item, c)
        return pltpu.make_async_remote_copy(
            src_ref=ref,
            dst_ref=ref,
            send_sem=send_sem.at[way, item, c],
            recv_sem=recv_sem.at[item, c],
            device_id={"rows": targets[way]},
            device_id_type=MESH,
        )

    def arrive(item, c):
        copy(item, c, SIDE).wait_recv()

    def crossing(c):
        return c in twice

    def merge(c):
        train, low, high, serve, start, length = chunks[c]
        rows = pl.ds(start, length)
        update = lax.dot_general(
            high[:, rows], low[...], (((0,), (0,)), ((), ())), preferred_element_type=jnp.float32
        )
        fresh = train[:, rows].T.astype(jnp.float32) + mix_rate * update
        serve[rows, pl.ds(pl.multiple_of(me * width, 128), width)] = fresh.astype(jnp.bfloat16)

    def send_own(c):
        @pl.when(has_down)
        def _():
            copy(me, c, DOWN).start()

        @pl.when(has_up)
        def _():
            copy(me, c, UP).start()

        copy(me, c, SIDE).start()

    def gain_copy(k):
        return pltpu.make_async_remote_copy(
            src_ref=gains.at[me, core],
            dst_ref=gains.at[me, core],
            send_sem=gain_send.at[k],
            recv_sem=gain_recv.at[k],
            device_id=partner(k),
            device_id_type=MESH,
        )

    for n in (0, 1, 2, 9, 10):
        loads[n].wait()
    gains[pl.ds(me, 1), pl.ds(core, 1)] = (norm_train[...] + norm_step[...])[None, None]
    merge(0)
    merge(1)
    pl.semaphore_wait(barrier, tp_size + has_up.astype(jnp.int32) + has_down.astype(jnp.int32))
    for c in range(2, count + 2):
        send_own(c - 2)
        if c < count:
            if c == queries:
                for n in range(3, 9):
                    loads[n].wait()
            merge(c)
        if c == 3:
            for k in range(1, tp_size):
                gain_copy(k).start()
    for k in range(1, tp_size):
        gain_copy(k).wait_recv()
    send_own(count)

    def pass_on(step, c):
        below, above = me - 2 * step, me + 2 * step

        @pl.when(z >= step)
        def _():
            arrive(below, c)

            @pl.when(has_up)
            def _():
                copy(below, c, UP).start()

            if not (step == 1 and crossing(c)):
                copy(below, c, SIDE).start()

        @pl.when(z + step < depth)
        def _():
            arrive(above, c)

            @pl.when(has_down)
            def _():
                copy(above, c, DOWN).start()

            if not (step == 1 and crossing(c)):
                copy(above, c, SIDE).start()

    def cross(c):
        arrive(side, c)

        @pl.when(has_down)
        def _():
            copy(side, c, DOWN).start()

        @pl.when(has_up)
        def _():
            copy(side, c, UP).start()

    for step in range(1, depth):
        for c in range(count + 1):
            pass_on(step, c)
        if step == max(1, depth - 2):
            for c in range(count):
                if crossing(c):
                    cross(c)

    for c in range(count + 1):
        if not crossing(c):
            arrive(side, c)
    for step in range(1, depth):
        for c in range(count + 1):
            @pl.when(z >= step)
            def _():
                arrive(side - 2 * step, c)

            @pl.when(z + step < depth)
            def _():
                arrive(side + 2 * step, c)

    serve_norm[...] = gains[...].reshape(serve_norm.shape).astype(jnp.bfloat16)

    for k in range(1, tp_size):
        gain_copy(k).wait_send()
    for c in range(count + 1):
        copy(me, c, SIDE).wait_send()

        @pl.when(has_down)
        def _():
            copy(me, c, DOWN).wait_send()
            if crossing(c):
                copy(side, c, DOWN).wait_send()

        @pl.when(has_up)
        def _():
            copy(me, c, UP).wait_send()
            if crossing(c):
                copy(side, c, UP).wait_send()

        for step in range(1, depth):
            below, above = me - 2 * step, me + 2 * step

            @pl.when(z >= step)
            def _():
                @pl.when(has_up)
                def _():
                    copy(below, c, UP).wait_send()

                if not (step == 1 and crossing(c)):
                    copy(below, c, SIDE).wait_send()

            @pl.when(z + step < depth)
            def _():
                @pl.when(has_down)
                def _():
                    copy(above, c, DOWN).wait_send()

                if not (step == 1 and crossing(c)):
                    copy(above, c, SIDE).wait_send()


def fused(size, tp_size, *args):
    train_query, train_key, train_value, norm_train = args[0], args[3], args[6], args[9]
    seats, norm_length = size * tp_size, norm_train.shape[0]
    args = [a.T if n in (1, 4, 7) else a for n, a in enumerate(args)]
    args = [a.reshape(1, -1) if a.ndim == 1 else a for a in args]
    full = train_query.shape[0] * size
    outs = [
        pltpu.VMEM((t.shape[1], full), jnp.bfloat16)
        for t in (train_query, train_key, train_value)
    ]
    outs.append(pltpu.VMEM((seats, norm_length), jnp.bfloat16))
    lengths = [t.shape[1] for t in (train_query, train_key, train_value)]
    count = sum(len(cuts(length, n == 0)) for n, length in enumerate(lengths))
    grant = VMEM_BYTES - 2 * (sum(t.shape[1] for t in (train_query, train_key, train_value)) * full)
    grant -= 2 * seats * norm_length
    vmem = pl.BlockSpec(memory_space=pltpu.VMEM)
    query, key, value, norm = pl.pallas_call(
        functools.partial(kernel, size, tp_size),
        out_shape=outs,
        in_specs=[pl.BlockSpec(memory_space=pltpu.HBM)] * 11,
        out_specs=[vmem] * 4,
        scratch_shapes=[pltpu.VMEM(a.shape, a.dtype) for a in args]
        + [
            pltpu.VMEM((size, tp_size, 1, norm_length), jnp.float32),
            pltpu.SemaphoreType.DMA((11,)),
            pltpu.SemaphoreType.DMA((3, size, count + 1)),
            pltpu.SemaphoreType.DMA((size, count + 1)),
            pltpu.SemaphoreType.DMA((tp_size,)),
            pltpu.SemaphoreType.DMA((tp_size,)),
        ],
        compiler_params=pltpu.CompilerParams(
            collective_id=0, has_side_effects=True, vmem_limit_bytes=grant
        ),
    )(*args)
    query, key, value, norm = store_out(query, key, value, norm)
    return query, key, value, norm.reshape(-1)


def store_kernel(*refs):
    ins, outs, sems = refs[:4], refs[4:8], refs[8]
    copies = [pltpu.make_async_copy(i, o, sems.at[n]) for n, (i, o) in enumerate(zip(ins, outs))]
    for c in copies:
        c.start()
    for c in copies:
        c.wait()


def store_out(*arrays):
    return pl.pallas_call(
        store_kernel,
        out_shape=[jax.ShapeDtypeStruct(a.shape, a.dtype) for a in arrays],
        in_specs=[pl.BlockSpec(memory_space=pltpu.VMEM)] * 4,
        out_specs=[pl.BlockSpec(memory_space=pltpu.HBM)] * 4,
        scratch_shapes=[pltpu.SemaphoreType.DMA((4,))],
        compiler_params=pltpu.CompilerParams(vmem_limit_bytes=16 * 2**20),
    )(*arrays)


def plain(
    train_query,
    low_query,
    high_query,
    train_key,
    low_key,
    high_key,
    train_value,
    low_value,
    high_value,
    norm_train,
    norm_step,
):
    def merged(train, low, high):
        update = jnp.dot(low, high, preferred_element_type=jnp.float32)
        fresh = train.astype(jnp.float32) + mix_rate * update
        return lax.all_gather(fresh.astype(jnp.bfloat16), "rows", axis=0, tiled=True).T

    serve_norm = lax.all_gather(
        (norm_train + norm_step).astype(jnp.bfloat16), ("rows", "tp"), axis=0, tiled=True
    )
    return (
        merged(train_query, low_query, high_query),
        merged(train_key, low_key, high_key),
        merged(train_value, low_value, high_value),
        serve_norm,
    )


def solution(mesh):
    size, tp_size = mesh.shape["rows"], mesh.shape["tp"]

    def local(*args):
        trains = (args[0], args[3], args[6])
        fits = (
            size % 2 == 0
            and size >= 4
            and all(t.shape[0] % 128 == 0 and t.shape[1] % FIRST_ROWS == 0 for t in trains)
            and args[9].shape[0] % 128 == 0
        )
        return fused(size, tp_size, *args) if fits else plain(*args)

    in_specs = (
        P(("job", "rows"), "tp"),
        P(("job", "rows"), None),
        P("job", "tp"),
        P(("job", "rows"), "tp"),
        P(("job", "rows"), None),
        P("job", "tp"),
        P(("job", "rows"), "tp"),
        P(("job", "rows"), None),
        P("job", "tp"),
        P(("job", "rows", "tp")),
        P(("job", "rows", "tp")),
    )
    out_specs = (P(("job", "tp"), None), P(("job", "tp"), None), P(("job", "tp"), None), P("job"))
    return jax.shard_map(local, mesh=mesh, in_specs=in_specs, out_specs=out_specs, check_vma=False)
```
